8 devices in a mesh: dp: 2 (over z, y), ep: 4 (over x, core).
Axes of the slice: x: 2, y: 2, z: 1, core: 2. Of those that a mesh axis runs over, the one named last changes fastest.
Arguments:
- x_tokens: bfloat16 [512, 1536], P(('dp', 'ep')), parts along dimension 0
- dy_tokens: bfloat16 [512, 1536], P(('dp', 'ep')), parts along dimension 0
- expert_ids: int32 [512, 8], P(('dp', 'ep')), parts along dimension 0
- gate_vals: float32 [512, 8], P(('dp', 'ep')), parts along dimension 0
- slot_ids: int32 [512, 8], P(('dp', 'ep')), parts along dimension 0
- w_gate: bfloat16 [40, 1536, 512], P('ep')
- w_down: bfloat16 [40, 512, 1536], P('ep')
- w_up: bfloat16 [40, 1536, 512], P('ep')
Outputs:
- output 1: bfloat16 [512, 1536], P(('dp', 'ep')), parts along dimension 0
- output 2: float32 [80, 1536, 512], P(('dp', 'ep')), parts along dimension 0
- output 3: float32 [80, 512, 1536], P(('dp', 'ep')), parts along dimension 0
- output 4: float32 [80, 1536, 512], P(('dp', 'ep')), parts along dimension 0
There are 2 independent parts. The reference program is written for one: setup_inputs(seed, part) draws one part's arguments, and reference() takes and returns one part's arrays. A program takes and returns all parts, laid end to end along the dimension named above; an argument that names none is the same for every part.
All inputs are finite; a program needn't handle non-finite values.
Results may differ from the reference program's by a relative error of at most 0.010384.
Values are sent between devices in bfloat16 or wider.
A program may use at most 1 GiB of HBM per device.

```python
import jax
import jax.numpy as jnp
from jax import lax

D = 1536
FF = 512
EXPERTS = 40
TOP = 8
GROUP = 4
TOK = 64
CAP = 24


def source_routing(src_key):
    key_base, key_offset, key_hot = jax.random.split(src_key, 3)
    stride = EXPERTS // TOP
    base_expert = jax.random.randint(key_base, (TOK,), 0, EXPERTS)
    offset = jax.random.randint(key_offset, (TOK, TOP), 0, stride)
    hot_expert = jax.random.randint(key_hot, (), 0, EXPERTS)
    forced = jnp.arange(TOK) < CAP
    base_expert = jnp.where(forced, hot_expert, base_expert)
    offset = jnp.where(forced[:, None] & (jnp.arange(TOP)[None, :] == 0), 0, offset)
    experts = (base_expert[:, None] + jnp.arange(TOP)[None, :] * stride + offset) % EXPERTS
    n_copy = TOK * TOP
    flat_exp = experts.reshape(n_copy)
    copy_ids = jnp.arange(n_copy)
    sort_order = jnp.argsort(flat_exp * n_copy + copy_ids)
    exp_counts = jnp.zeros((EXPERTS,), jnp.int32).at[flat_exp].add(1)
    exp_starts = jnp.cumsum(exp_counts) - exp_counts
    sorted_rank = copy_ids - exp_starts[flat_exp[sort_order]]
    copy_rank = jnp.zeros((n_copy,), jnp.int32).at[sort_order].set(sorted_rank)
    slots = jnp.where(copy_rank < CAP, copy_rank, -1)
    return experts.astype(jnp.int32), slots.reshape(TOK, TOP).astype(jnp.int32)


def setup_inputs(seed: int = 0, part: int = 0) -> dict:
    root_key = jax.random.key(seed)
    sub_keys = jax.random.split(root_key, 7)
    n_tok = GROUP * TOK
    x_tokens = jax.random.normal(jax.random.fold_in(sub_keys[0], part), (n_tok, D), jnp.float32).astype(jnp.bfloat16)
    dy_tokens = jax.random.normal(jax.random.fold_in(sub_keys[1], part), (n_tok, D), jnp.float32).astype(jnp.bfloat16)
    gate_vals = jax.random.uniform(jax.random.fold_in(sub_keys[2], part), (n_tok, TOP), jnp.float32, 0.3, 1.0)
    src_keys = jax.random.split(jax.random.fold_in(sub_keys[3], part), GROUP)
    expert_ids, slot_ids = jax.vmap(source_routing)(src_keys)
    w_gate = (jax.random.normal(sub_keys[4], (EXPERTS, D, FF), jnp.float32) * D ** -0.5).astype(jnp.bfloat16)
    w_down = (jax.random.normal(sub_keys[5], (EXPERTS, FF, D), jnp.float32) * FF ** -0.5).astype(jnp.bfloat16)
    w_up = (jax.random.normal(sub_keys[6], (EXPERTS, D, FF), jnp.float32) * D ** -0.5).astype(jnp.bfloat16)
    return {'x_tokens': x_tokens, 'dy_tokens': dy_tokens, 'expert_ids': expert_ids.reshape(n_tok, TOP), 'gate_vals': gate_vals, 'slot_ids': slot_ids.reshape(n_tok, TOP), 'w_gate': w_gate, 'w_down': w_down, 'w_up': w_up}


def expert_backward(operands):
    x_rows, dz_rows, w_gate, w_down, w_up = operands
    a_pre = jnp.dot(x_rows, w_gate, preferred_element_type=jnp.float32).astype(jnp.bfloat16).astype(jnp.float32)
    b_pre = jnp.dot(x_rows, w_up, preferred_element_type=jnp.float32).astype(jnp.bfloat16).astype(jnp.float32)
    sigma_a = jax.nn.sigmoid(a_pre)
    silu_a = a_pre * sigma_a
    hidden = (silu_a * b_pre).astype(jnp.bfloat16)
    d_hidden = jnp.dot(dz_rows, w_down.T, preferred_element_type=jnp.float32)
    d_gate = (d_hidden * b_pre * sigma_a * (1.0 + a_pre * (1.0 - sigma_a))).astype(jnp.bfloat16)
    d_up = (d_hidden * silu_a).astype(jnp.bfloat16)
    g_down = jnp.dot(hidden.T, dz_rows, preferred_element_type=jnp.float32)
    g_gate = jnp.dot(x_rows.T, d_gate, preferred_element_type=jnp.float32)
    g_up = jnp.dot(x_rows.T, d_up, preferred_element_type=jnp.float32)
    dx_rows = (jnp.dot(d_gate, w_gate.T, preferred_element_type=jnp.float32) + jnp.dot(d_up, w_up.T, preferred_element_type=jnp.float32)).astype(jnp.bfloat16)
    return dx_rows, g_gate, g_down, g_up


def reference(x_tokens, dy_tokens, expert_ids, gate_vals, slot_ids, w_gate, w_down, w_up):
    n_tok = GROUP * TOK
    n_rows = GROUP * CAP
    n_slot = EXPERTS * n_rows
    source = jnp.arange(n_tok) // TOK
    buf_index = jnp.where(slot_ids >= 0, expert_ids * n_rows + source[:, None] * CAP + slot_ids, n_slot)
    slot_copy = jnp.full((n_slot,), n_tok * TOP, jnp.int32).at[buf_index.reshape(n_tok * TOP)].set(jnp.arange(n_tok * TOP, dtype=jnp.int32), mode='drop')
    slot_tok = slot_copy // TOP
    x_buf = jnp.take(x_tokens, slot_tok, axis=0, mode='fill', fill_value=0).reshape(EXPERTS, n_rows, D)
    gate_slot = jnp.take(gate_vals.reshape(n_tok * TOP), slot_copy, mode='fill', fill_value=0)
    dy_slot = jnp.take(dy_tokens, slot_tok, axis=0, mode='fill', fill_value=0)
    dz_buf = (gate_slot[:, None] * dy_slot).astype(jnp.bfloat16).reshape(EXPERTS, n_rows, D)
    dx_buf, dw_gate, dw_down, dw_up = lax.map(expert_backward, (x_buf, dz_buf, w_gate, w_down, w_up))
    returned = jnp.take(dx_buf.reshape(n_slot, D), buf_index, axis=0, mode='fill', fill_value=0)
    dx_tokens = jnp.sum(returned.astype(jnp.float32), axis=1).astype(jnp.bfloat16)
    return (dx_tokens, dw_gate, dw_down, dw_up)
```

```python
import functools

import jax
import jax.numpy as jnp
from jax import lax
from jax.experimental import pallas as pl
from jax.experimental.pallas import tpu as pltpu
from jax.sharding import PartitionSpec as P

F32, BF16 = jnp.float32, jnp.bfloat16
TN = (((0,), (0,)), ((), ()))
NT = (((1,), (1,)), ((), ()))


def slot_capacity(tok_dev, top_k, n_exp):
    return ((3 * tok_dev * top_k) // (2 * n_exp) + 7) // 8 * 8


def dot(a, b, dims=None):
    if dims is None:
        return jnp.dot(a, b, preferred_element_type=F32)
    return lax.dot_general(a, b, dims, preferred_element_type=F32)


def build_rows(cap, tok_dev, n_dev, n_local, key_ref, gate_ref, x_ref, dy_ref, hot, x_all, dz_all):
    rows = n_dev * cap
    n_tok = n_dev * tok_dev
    first = lax.axis_index('ep') * n_local
    keys = key_ref[...]
    gates = gate_ref[...]
    source = lax.broadcasted_iota(jnp.int32, (1, n_tok), 1) // tok_dev * cap
    row_ids = lax.broadcasted_iota(jnp.int32, (rows, n_tok), 0)
    for e in range(n_local):
        d = keys - (first + e) * cap
        hit = (d >= 0) & (d < cap)
        slot = jnp.sum(jnp.where(hit, d + 1, 0), axis=0, keepdims=True) - 1
        gmap = jnp.sum(jnp.where(hit, gates, 0.0), axis=0, keepdims=True)
        slot = jnp.where(slot >= 0, slot + source, -1)
        mask = row_ids == slot
        gcol = jnp.sum(jnp.where(mask, gmap, 0.0), axis=1, keepdims=True)
        sel = jnp.where(mask, 1.0, 0.0).astype(BF16)
        hot[pl.ds(e * rows, rows), :] = sel
        x_all[e] = dot(sel, x_ref[...]).astype(BF16)
        dz_all[e] = (gcol * dot(sel, dy_ref[...])).astype(BF16)


def expert_kernel(cfg, key_ref, gate_ref, x_ref, dy_ref, w1_ref, w2_ref, w3_ref,
                  part_ref, dw1_ref, dw2_ref, dw3_ref, hot, x_all, dz_all, dx_all):
    cap, tok_dev, n_dev, n_local = cfg
    rows = n_dev * cap
    i = pl.program_id(0)

    @pl.when(i == 0)
    def _():
        build_rows(cap, tok_dev, n_dev, n_local, key_ref, gate_ref, x_ref, dy_ref, hot, x_all, dz_all)

    x = x_all[i]
    dz = dz_all[i]
    a = dot(x, w1_ref[0]).astype(BF16).astype(F32)
    b = dot(x, w3_ref[0]).astype(BF16).astype(F32)
    sg = jax.nn.sigmoid(a)
    silu = a * sg
    h = (silu * b).astype(BF16)
    dh = dot(dz, w2_ref[0], NT)
    da = (dh * b * sg * (1.0 + a * (1.0 - sg))).astype(BF16)
    db = (dh * silu).astype(BF16)
    dx = (dot(da, w1_ref[0], NT) + dot(db, w3_ref[0], NT)).astype(BF16)
    dx_all[pl.ds(pl.multiple_of(i * rows, 16), rows), :] = dx
    d_model = x.shape[1]
    ff = h.shape[1]
    for c in range(d_model // 256):
        xt = x_all[i, :, pl.ds(c * 256, 256)]
        dw1_ref[0, pl.ds(c * 256, 256), :] = dot(xt, da, TN)
        dw3_ref[0, pl.ds(c * 256, 256), :] = dot(xt, db, TN)
    for c in range(ff // 256):
        dw2_ref[0, pl.ds(c * 256, 256), :] = dot(h[:, c * 256:(c + 1) * 256], dz, TN)

    @pl.when(i == n_local - 1)
    def _():
        part_ref[...] = dot(hot[...], dx_all[...], TN)


def solution(mesh):
    n_dev = mesh.shape['ep']

    def local_step(x_loc, dy_loc, ids_loc, gate_loc, slot_loc, w_gate, w_down, w_up):
        tok_dev, top_k = ids_loc.shape
        n_local, d_model, ff = w_gate.shape
        n_exp = n_local * n_dev
        n_tok = tok_dev * n_dev
        cap = slot_capacity(tok_dev, top_k, n_exp)
        rows = n_dev * cap
        keys = jnp.where(slot_loc >= 0, ids_loc * cap + slot_loc, -1).T
        keys = lax.all_gather(keys, 'ep', axis=1, tiled=True)
        gates = lax.all_gather(gate_loc.T, 'ep', axis=1, tiled=True)
        x_tok = lax.all_gather(x_loc, 'ep', axis=0, tiled=True)
        dy_tok = lax.all_gather(dy_loc, 'ep', axis=0, tiled=True)
        whole = lambda shape: pl.BlockSpec(shape, lambda i: (0,) * len(shape))
        per = lambda shape: pl.BlockSpec((1,) + shape, lambda i: (i, 0, 0))
        part, g1, g2, g3 = pl.pallas_call(
            functools.partial(expert_kernel, (cap, tok_dev, n_dev, n_local)),
            grid=(n_local,),
            out_shape=[
                jax.ShapeDtypeStruct((n_tok, d_model), F32),
                jax.ShapeDtypeStruct((n_local, d_model, ff), F32),
                jax.ShapeDtypeStruct((n_local, ff, d_model), F32),
                jax.ShapeDtypeStruct((n_local, d_model, ff), F32),
            ],
            in_specs=[whole((top_k, n_tok)), whole((top_k, n_tok)), whole((n_tok, d_model)), whole((n_tok, d_model)),
                      per((d_model, ff)), per((ff, d_model)), per((d_model, ff))],
            out_specs=[whole((n_tok, d_model)), per((d_model, ff)), per((ff, d_model)), per((d_model, ff))],
            scratch_shapes=[
                pltpu.VMEM((n_local * rows, n_tok), BF16),
                pltpu.VMEM((n_local, rows, d_model), BF16),
                pltpu.VMEM((n_local, rows, d_model), BF16),
                pltpu.VMEM((n_local * rows, d_model), BF16),
            ],
            compiler_params=pltpu.CompilerParams(dimension_semantics=('arbitrary',), vmem_limit_bytes=62 * 1024 * 1024),
            cost_estimate=pl.CostEstimate(flops=16 * n_local * rows * d_model * ff, bytes_accessed=18 * n_local * d_model * ff, transcendentals=0),
            name='experts',
        )(keys, gates, x_tok, dy_tok, w_gate, w_down, w_up)
        dx = lax.psum_scatter(part, 'ep', scatter_dimension=0, tiled=True).astype(BF16)
        return dx, g1, g2, g3

    tok_spec = P(('dp', 'ep'), None)
    w_spec = P('ep', None, None)
    grad_spec = P(('dp', 'ep'), None, None)
    return jax.shard_map(local_step, mesh=mesh, in_specs=(tok_spec, tok_spec, tok_spec, tok_spec, tok_spec, w_spec, w_spec, w_spec), out_specs=(tok_spec, grad_spec, grad_spec, grad_spec), check_vma=False)
```

```python
import functools

import jax
import jax.numpy as jnp
import numpy as np
from jax import lax
from jax.experimental import pallas as pl
from jax.experimental.pallas import tpu as pltpu
from jax.sharding import PartitionSpec as P

F32, BF16 = jnp.float32, jnp.bfloat16
MESH = pl.DeviceIdType.MESH
TN = (((0,), (0,)), ((), ()))
NT = (((1,), (1,)), ((), ()))
DONE_FIRST = 5
SECOND = 1
MIB = 1024 * 1024


def slot_capacity(tok_dev, top_k, n_exp):
    return ((3 * tok_dev * top_k) // (2 * n_exp) + 7) // 8 * 8


def dot(a, b, dims=None):
    if dims is None:
        return jnp.dot(a, b, preferred_element_type=F32)
    return lax.dot_general(a, b, dims, preferred_element_type=F32)


def gather_kernel(meta_ref, x_ref, dy_ref, meta_out, x_out, dy_out, send_sem, recv_sem):
    dp, me = lax.axis_index('dp'), lax.axis_index('ep')
    partner = me + 1 - 2 * lax.rem(me, 2)
    twin = lax.rem(me + 2, 4)
    barrier = pltpu.get_barrier_semaphore()
    for peer in (partner, twin):
        pl.semaphore_signal(barrier, inc=1, device_id=(dp, peer), device_id_type=MESH)
    pl.semaphore_wait(barrier, 2)

    def copy(src, dst, slot, peer, k):
        return pltpu.make_async_remote_copy(src_ref=src, dst_ref=dst.at[slot], send_sem=send_sem.at[k], recv_sem=recv_sem.at[k],
                                            device_id=(dp, peer), device_id_type=MESH)

    pairs = ((meta_ref, meta_out), (x_ref, x_out), (dy_ref, dy_out))
    cross = [copy(src, dst, me, twin, 3 * n) for n, (src, dst) in enumerate(pairs)]
    near = [copy(src, dst, me, partner, 3 * n + 1) for n, (src, dst) in enumerate(pairs)]
    for c in cross:
        c.start()
    for c in near:
        c.start()
    for src, dst in pairs:
        dst[me] = src[...]
    onward = []
    for n, (src, dst) in enumerate(pairs):
        cross[n].wait_recv()
        c = copy(dst.at[twin], dst, twin, partner, 3 * n + 2)
        c.start()
        onward.append(c)
    for c in near + onward:
        c.wait_recv()
    for c in cross + near + onward:
        c.wait_send()


def gather_tokens(meta, x_loc, dy_loc, n_dev):
    vmem = pl.BlockSpec(memory_space=pltpu.VMEM)
    args = (meta, x_loc, dy_loc)
    return pl.pallas_call(
        gather_kernel,
        out_shape=[jax.ShapeDtypeStruct((n_dev,) + a.shape, a.dtype) for a in args],
        in_specs=[vmem] * 3,
        out_specs=[vmem] * 3,
        scratch_shapes=[pltpu.SemaphoreType.DMA((9,)), pltpu.SemaphoreType.DMA((9,))],
        compiler_params=pltpu.CompilerParams(collective_id=0, has_side_effects=True, vmem_limit_bytes=8 * MIB),
        name='gather_tokens',
    )(*args)


def build_rows(cfg, meta_ref, x_ref, dy_ref, hot, x_all, dz_all):
    cap, tok_dev, n_dev, n_local, top_k = cfg
    rows, n_tok = n_dev * cap, n_dev * tok_dev
    me = lax.axis_index('ep')
    first = me * n_local
    keys = jnp.concatenate([meta_ref[s, :top_k, :] for s in range(n_dev)], axis=1)
    gates = jnp.concatenate([meta_ref[s, top_k:, :] for s in range(n_dev)], axis=1)
    keys = keys.astype(jnp.int32)
    source = lax.broadcasted_iota(jnp.int32, (1, n_tok), 1) // tok_dev * cap
    row_ids = lax.broadcasted_iota(jnp.int32, (rows, n_tok), 0)
    x = x_ref[...].reshape(n_tok, -1)
    dy = dy_ref[...].reshape(n_tok, -1)
    for e in range(n_local):
        d = keys - (first + e) * cap
        hit = (d >= 0) & (d < cap)
        slot = jnp.sum(jnp.where(hit, d + 1, 0), axis=0, keepdims=True) - 1
        gmap = jnp.sum(jnp.where(hit, gates, 0.0), axis=0, keepdims=True)
        slot = jnp.where(slot >= 0, slot + source, -1)
        mask = row_ids == slot
        gcol = jnp.sum(jnp.where(mask, gmap, 0.0), axis=1, keepdims=True)
        sel = jnp.where(mask, 1.0, 0.0).astype(BF16)
        hot[pl.ds(e * rows, rows), :] = sel
        x_all[e] = dot(sel, x).astype(BF16)
        dz_all[e] = (gcol * dot(sel, dy)).astype(BF16)


def weight_grads(x_ref, dz, h, da, db, dw1_ref, dw2_ref, dw3_ref):
    for c in range(dw1_ref.shape[1] // 256):
        xt = x_ref[:, pl.ds(c * 256, 256)]
        dw1_ref[0, pl.ds(c * 256, 256), :] = dot(xt, da, TN)
        dw3_ref[0, pl.ds(c * 256, 256), :] = dot(xt, db, TN)
    for c in range(dw2_ref.shape[1] // 256):
        dw2_ref[0, pl.ds(c * 256, 256), :] = dot(h[:, c * 256:(c + 1) * 256], dz, TN)


def first_kernel(cfg, expert_of, grad_of, save_of, flag_of, meta_ref, x_ref, dy_ref, w1_ref, w2_ref, w3_ref,
                 keep_ref, send_ref, xs_ref, dzs_ref, hs_ref, das_ref, dbs_ref, dw1_ref, dw2_ref, dw3_ref, hot, x_all, dz_all, dx_all):
    cap, tok_dev, n_dev, n_local, top_k = cfg
    rows = n_dev * cap
    i = pl.program_id(0)
    e = expert_of[i]

    @pl.when(i == 0)
    def _():
        build_rows(cfg, meta_ref, x_ref, dy_ref, hot, x_all, dz_all)

    x = x_all[e]
    dz = dz_all[e]
    a = dot(x, w1_ref[0]).astype(BF16).astype(F32)
    b = dot(x, w3_ref[0]).astype(BF16).astype(F32)
    sg = jax.nn.sigmoid(a)
    silu = a * sg
    h = (silu * b).astype(BF16)
    dh = dot(dz, w2_ref[0], NT)
    da = (dh * b * sg * (1.0 + a * (1.0 - sg))).astype(BF16)
    db = (dh * silu).astype(BF16)
    dx = (dot(da, w1_ref[0], NT) + dot(db, w3_ref[0], NT)).astype(BF16)
    dx_all[pl.ds(pl.multiple_of(e * rows, 16), rows), :] = dx

    @pl.when(flag_of[i] == 1)
    def _():
        weight_grads(x_all.at[e], dz, h, da, db, dw1_ref, dw2_ref, dw3_ref)

    @pl.when(flag_of[i] == 0)
    def _():
        xs_ref[0] = x
        dzs_ref[0] = dz
        hs_ref[0] = h
        das_ref[0] = da
        dbs_ref[0] = db

    @pl.when(i == n_local - 1)
    def _():
        me = lax.axis_index('ep')
        for s in range(n_dev):
            part = dot(hot[:, s * tok_dev:(s + 1) * tok_dev], dx_all[...], TN)
            q = jnp.bitwise_xor(s, me)
            half = q // 2

            @pl.when(q % 2 == 0)
            def _():
                keep_ref[half] = part

            @pl.when(q % 2 == 1)
            def _():
                send_ref[half] = part


def later_kernel(x_ref, dz_ref, h_ref, da_ref, db_ref, i1, i2, i3, dw1_ref, dw2_ref, dw3_ref):
    weight_grads(x_ref.at[0], dz_ref[0], h_ref[0], da_ref[0], db_ref[0], dw1_ref, dw2_ref, dw3_ref)


def grads_cost(n, rows, d_model, ff):
    return pl.CostEstimate(flops=6 * n * rows * d_model * ff, bytes_accessed=12 * n * d_model * ff, transcendentals=0)


def later_grads(saved, grads, start, first, count):
    rows, d_model = saved[0].shape[1:]
    ff = saved[2].shape[2]
    src = lambda shape: pl.BlockSpec((1,) + shape, lambda i: (start + i, 0, 0))
    dst = lambda shape: pl.BlockSpec((1,) + shape, lambda i: (first + start + i, 0, 0))
    return pl.pallas_call(
        later_kernel,
        grid=(count,),
        out_shape=[jax.ShapeDtypeStruct(g.shape, g.dtype) for g in grads],
        in_specs=[src((rows, d_model)), src((rows, d_model)), src((rows, ff)), src((rows, ff)), src((rows, ff))] + [pl.BlockSpec(memory_space=pl.ANY)] * 3,
        out_specs=[dst((d_model, ff)), dst((ff, d_model)), dst((d_model, ff))],
        input_output_aliases={5: 0, 6: 1, 7: 2},
        compiler_params=pltpu.CompilerParams(dimension_semantics=('arbitrary',), vmem_limit_bytes=32 * MIB),
        cost_estimate=grads_cost(count, rows, d_model, ff),
        name='later_grads',
    )(*saved, *grads)


def schedule(n_local, done):
    flags, acc = [], 0
    for i in range(n_local):
        acc += done
        flags.append(1 if acc >= n_local or i == 0 and done else 0)
        if flags[-1]:
            acc -= n_local
    while sum(flags) > done:
        flags[len(flags) - 1 - flags[::-1].index(1)] = 0
    n_done = n_save = 0
    expert, grad, save = [], [], []
    for f in flags:
        expert.append(n_done if f else done + n_save)
        grad.append(min(n_done, max(done - 1, 0)))
        save.append(min(n_save, max(n_local - done - 1, 0)))
        n_done += f
        n_save += 1 - f
    return [np.asarray(v, np.int32) for v in (expert, grad, save, flags)]


def first_experts(cfg, meta, x_tok, dy_tok, w_gate, w_down, w_up, done):
    cap, tok_dev, n_dev, n_local, top_k = cfg
    d_model, ff = w_gate.shape[1:]
    rows, n_tok, left = n_dev * cap, n_dev * tok_dev, n_local - done
    vmem = pl.BlockSpec(memory_space=pltpu.VMEM)
    per = lambda shape: pl.BlockSpec((1,) + shape, lambda i, ex, gr, sa, fl: (ex[i], 0, 0))
    grad = lambda shape: pl.BlockSpec((1,) + shape, lambda i, ex, gr, sa, fl: (gr[i], 0, 0))
    save = lambda shape: pl.BlockSpec((1,) + shape, lambda i, ex, gr, sa, fl: (sa[i], 0, 0))
    out = jax.ShapeDtypeStruct
    return pl.pallas_call(
        functools.partial(first_kernel, cfg),
        grid_spec=pltpu.PrefetchScalarGridSpec(
            num_scalar_prefetch=4,
            grid=(n_local,),
            in_specs=[vmem, vmem, vmem, per((d_model, ff)), per((ff, d_model)), per((d_model, ff))],
            out_specs=[vmem, vmem, save((rows, d_model)), save((rows, d_model)), save((rows, ff)), save((rows, ff)), save((rows, ff)),
                       grad((d_model, ff)), grad((ff, d_model)), grad((d_model, ff))],
            scratch_shapes=[
                pltpu.VMEM((n_local * rows, n_tok), BF16),
                pltpu.VMEM((n_local, rows, d_model), BF16),
                pltpu.VMEM((n_local, rows, d_model), BF16),
                pltpu.VMEM((n_local * rows, d_model), BF16),
            ],
        ),
        out_shape=[
            out((2, tok_dev, d_model), F32), out((2, tok_dev, d_model), F32),
            out((left, rows, d_model), BF16), out((left, rows, d_model), BF16), out((left, rows, ff), BF16), out((left, rows, ff), BF16), out((left, rows, ff), BF16),
            out((n_local, d_model, ff), F32), out((n_local, ff, d_model), F32), out((n_local, d_model, ff), F32),
        ],
        compiler_params=pltpu.CompilerParams(dimension_semantics=('arbitrary',), vmem_limit_bytes=46 * MIB),
        cost_estimate=pl.CostEstimate(flops=16 * n_local * rows * d_model * ff, bytes_accessed=12 * n_local * d_model * ff, transcendentals=0),
        name='first_experts',
    )(*schedule(n_local, done), meta, x_tok, dy_tok, w_gate, w_down, w_up)


def solution(mesh):
    n_dev = mesh.shape['ep']

    def local_step(x_loc, dy_loc, ids_loc, gate_loc, slot_loc, w_gate, w_down, w_up):
        tok_dev, top_k = ids_loc.shape
        n_local, d_model, ff = w_gate.shape
        cap = slot_capacity(tok_dev, top_k, n_local * n_dev)
        cfg = (cap, tok_dev, n_dev, n_local, top_k)
        keys = jnp.where(slot_loc >= 0, ids_loc * cap + slot_loc, -1).astype(F32)
        meta = jnp.concatenate([keys.T, gate_loc.T], axis=0)
        meta, x_tok, dy_tok = gather_tokens(meta, x_loc, dy_loc, n_dev)
        done = DONE_FIRST
        keep, send, *rest = first_experts(cfg, meta, x_tok, dy_tok, w_gate, w_down, w_up, done)
        saved, grads = rest[:5], rest[5:]
        got = lax.ppermute(send, 'ep', [(d, d ^ 1) for d in range(n_dev)])
        grads = later_grads(saved, grads, 0, done, SECOND)
        cross = lax.ppermute(keep[1] + got[1], 'ep', [(d, d ^ 2) for d in range(n_dev)])
        grads = later_grads(saved, grads, SECOND, done, n_local - done - SECOND)
        dx = (keep[0] + got[0] + cross).astype(BF16)
        return dx, *grads

    tok_spec = P(('dp', 'ep'), None)
    w_spec = P('ep', None, None)
    grad_spec = P(('dp', 'ep'), None, None)
    return jax.shard_map(local_step, mesh=mesh, in_specs=(tok_spec, tok_spec, tok_spec, tok_spec, tok_spec, w_spec, w_spec, w_spec), out_specs=(tok_spec, grad_spec, grad_spec, grad_spec), check_vma=False)
```
